32 devices in a mesh: blk: 16 (over z, y, core), head: 2 (over x).
Axes of the slice: x: 2, y: 2, z: 4, core: 2. Of those that a mesh axis runs over, the one named last changes fastest.
Arguments:
- queries: bfloat16 [4096, 1024], P('blk', 'head'), may hold values from -216 to 216
- keys: bfloat16 [4096, 1024], P('blk', 'head'), may hold values from -6 to 6
- values: bfloat16 [4096, 1024], P('blk', 'head'), may hold values from -6 to 6
- group_table: int32 [16, 2], P('blk'), may hold values from 0 to 31, as said below
- doc_ids: int32 [4096], replicated, may hold values from 0 to 15, never falling along the last dimension, each value on 1 to 2048 neighbouring positions
Outputs:
- attended: bfloat16 [4096, 1024], P('blk', 'head')
The draws below stay inside these ranges and needn't reach their ends.
Inputs may be any that keep to these rules, and one draw needn't show every extreme that they name: group_table[d, 1] = 31 - group_table[d, 0]; the first column holds each of 0 to 15 once. `doc_ids`: document numbers never fall along positions; a document holds at most 2048 positions.
All inputs are finite; a program needn't handle non-finite values.
Results may differ from the reference program's by a relative error of at most 0.0049.
Values may be sent and summed in bfloat16 or wider, within the bound.
A program may use at most 192 MiB of HBM per device.

```python
import math
import jax
import jax.numpy as jnp
import numpy as np
from jax import lax

HEAD_DIM = 128
HEADS = 8
TOK_DEV = 256
DOCS = 16
GROUP = 128
SEQ = 4096
MAXDOC = 2048
N_BLK = 16


def draw_queries(key, part):
    drawn = jnp.clip(jax.random.normal(jax.random.fold_in(key, 11), (SEQ, HEADS, HEAD_DIM), jnp.float32), -6.0, 6.0)
    return drawn.reshape(SEQ, HEADS * HEAD_DIM).astype(jnp.bfloat16)


def draw_keys(key, part):
    drawn = jnp.clip(jax.random.normal(jax.random.fold_in(key, 13), (SEQ, HEADS, HEAD_DIM), jnp.float32), -6.0, 6.0)
    return drawn.reshape(SEQ, HEADS * HEAD_DIM).astype(jnp.bfloat16)


def draw_group_table(key, part):
    order = jax.random.permutation(jax.random.fold_in(key, 17), N_BLK).astype(jnp.int32)
    return jnp.stack([order, 2 * N_BLK - 1 - order], axis=1).astype(jnp.int32)


def steps_of(key, extent, pieces, low, high):
    def one(dim, shards_of):
        heights = jax.random.uniform(jax.random.fold_in(jax.random.fold_in(key, 6), dim), (shards_of,), jnp.float32, low / len(pieces), high / len(pieces))
        return jnp.repeat(jnp.exp(heights), extent[dim] // shards_of).reshape((-1,) + (1,) * (len(extent) - dim - 1))

    loudness = one(*pieces[0])
    for cut in pieces[1:]:
        loudness = loudness * one(*cut)
    return loudness


def length_profile(amount, total, most, slope):
    loads = [(1 << 20) // math.isqrt(grade ** slope) + 1 for grade in range(2, amount + 1)]
    surplus, holding = total - most - (amount - 1), [1] * (amount - 1)
    while surplus > 0:
        candidates = [i for i in range(amount - 1) if holding[i] < most]
        whole, remaining = sum([loads[i] for i in candidates]), surplus
        for i in candidates:
            extra = min(most - holding[i], max(1, remaining * loads[i] // whole), surplus)
            holding[i] = holding[i] + extra
            surplus = surplus - extra
    return np.array([most] + holding)


def uneven(stream_key, count, total, most, slope):
    if count == 2:
        one = jax.random.randint(stream_key, (), max(1, total - most), min(most, total - 1) + 1)
        return jnp.stack([one, total - one])
    tallies = jnp.asarray(length_profile(count, total, most, slope), jnp.int32)
    twos = (count - 1) // 2
    donor, taker = tallies[1:1 + 2 * twos:2], tallies[2:2 + 2 * twos:2]
    margin = jnp.minimum(donor - 1, most - taker)
    passed = jax.random.randint(jax.random.fold_in(stream_key, 1), (twos,), 0, 1 << 20) % (margin + 1)
    tallies = tallies.at[1:1 + 2 * twos:2].set(donor - passed).at[2:2 + 2 * twos:2].set(taker + passed)
    return tallies[jax.random.permutation(jax.random.fold_in(stream_key, 2), count)]


def noise(rng, extent, deviation, reach, pieces=(), kind=jnp.bfloat16):
    values = jax.random.normal(rng, extent, jnp.float32) * deviation
    if len(pieces) > 0:
        values = steps_of(rng, extent, pieces, -0.22, 0.18) * values
    return jnp.clip(values, min=-reach, max=reach).astype(kind)


def setup_inputs(seed: int = 0) -> dict:
    streams_of = jax.random.split(jax.random.key(seed), 6)
    return {
        "queries": draw_queries(jax.random.fold_in(streams_of[5], 71), 0),
        "keys": draw_keys(jax.random.fold_in(streams_of[5], 71), 0),
        "values": noise(streams_of[2], (SEQ, HEADS * HEAD_DIM), 1.0, 6.0, ((0, 16), (1, 2))),
        "group_table": draw_group_table(jax.random.fold_in(streams_of[5], 71), 0),
        "doc_ids": jnp.searchsorted(jnp.cumsum(uneven(streams_of[4], DOCS, SEQ, MAXDOC, 2)), jnp.arange(SEQ), side="right").astype(jnp.int32),
    }


def reference(queries, keys, values, group_table, doc_ids):
    row_ids = jnp.arange(SEQ, dtype=jnp.int32)
    device = row_ids // TOK_DEV
    slot_ids = row_ids % TOK_DEV // GROUP
    position = (group_table[device, slot_ids] * GROUP + row_ids % GROUP).astype(jnp.int32)
    document = doc_ids[position]
    score_scale = 1.0 / math.sqrt(HEAD_DIM)
    query_block = math.gcd(SEQ, 1024)
    block_count = SEQ // query_block

    def one_head(head_index):
        start = (head_index * HEAD_DIM).astype(jnp.int32)
        head_queries = lax.dynamic_slice_in_dim(queries, start, HEAD_DIM, 1)
        head_keys = lax.dynamic_slice_in_dim(keys, start, HEAD_DIM, 1)
        head_values = lax.dynamic_slice_in_dim(values, start, HEAD_DIM, 1)

        def attend_block(args):
            query_rows, block_pos, block_doc = args
            scores = jnp.dot(query_rows, head_keys.T, preferred_element_type=jnp.float32) * score_scale
            visible = (block_doc[:, None] == document[None, :]) & (position[None, :] <= block_pos[:, None])
            rowmax = lax.optimization_barrier(jnp.max(jnp.where(visible, scores, -jnp.inf), axis=1))
            weights = jnp.where(visible, jnp.exp(scores - rowmax[:, None]), 0.0)
            denominator = lax.optimization_barrier(jnp.sum(weights, axis=1))
            output = jnp.dot(weights.astype(jnp.bfloat16), head_values, preferred_element_type=jnp.float32)
            return output / denominator[:, None]
        blocks = (head_queries.reshape(block_count, query_block, HEAD_DIM), position.reshape(block_count, query_block), document.reshape(block_count, query_block))
        return lax.map(attend_block, blocks).reshape(SEQ, HEAD_DIM)
    outputs = lax.map(one_head, jnp.arange(HEADS, dtype=jnp.int32))
    return jnp.transpose(outputs, (1, 0, 2)).reshape(SEQ, HEADS * HEAD_DIM).astype(jnp.bfloat16)
```

```python
import functools
import math

import jax
import jax.numpy as jnp
from jax import lax
from jax.experimental import pallas as pl
from jax.experimental.pallas import tpu as pltpu
from jax.sharding import PartitionSpec as P

HEAD_DIM = 128
CORES = 2
LANES = 2


def attend_kernel(
    line, q_ref, k_ref, v_ref, pos_ref, low_ref, high_ref, out_ref,
    kv, posb, top, total, acc, recv, precv, own_send, own_psend, send, psend,
):
    rows, cols = k_ref.shape
    heads = cols // HEAD_DIM
    group = rows // 2
    factor = math.log2(math.e) / math.sqrt(HEAD_DIM)
    me = lax.axis_index("blk")
    core = lax.rem(me, CORES)
    lane = lax.rem(me // CORES, LANES)
    z = me // (CORES * LANES)

    def index(zz, yy, cc):
        return (zz * LANES + yy) * CORES + cc

    across = index(z, 1 - lane, core)
    partner = index(z, lane, 1 - core)
    ahead = index(z + 1, lane, core)
    behind = index(z - 1, lane, core)
    has_ahead = z + 1 < line
    has_behind = z >= 1

    short = rows // 8
    half = (rows - short) // 2
    pieces = ((0, short), (short, half), (short + half, half))

    barrier = pltpu.get_barrier_semaphore()

    def greet(target):
        pl.semaphore_signal(barrier, inc=1, device_id={"blk": target})

    greet(across)
    greet(partner)
    pl.when(has_ahead)(lambda: greet(ahead))
    pl.when(has_behind)(lambda: greet(behind))
    pl.semaphore_wait(barrier, 2 + has_ahead.astype(jnp.int32) + has_behind.astype(jnp.int32))

    def remote(src, dst, ssem, rsem, target):
        return pltpu.make_async_remote_copy(
            src_ref=src, dst_ref=dst, send_sem=ssem, recv_sem=rsem, device_id={"blk": target}
        )

    def own_copies(piece, kind, target):
        start, size = pieces[piece]
        part = pl.ds(start, size)
        found = [
            remote(k_ref.at[part], kv.at[me, part, pl.ds(0, cols)], own_send.at[piece, 0, kind], recv.at[me, piece], target),
            remote(v_ref.at[part], kv.at[me, part, pl.ds(cols, cols)], own_send.at[piece, 1, kind], recv.at[me, piece], target),
        ]
        if piece == 1:
            found.append(remote(pos_ref, posb.at[me], own_psend.at[kind], precv.at[me], target))
        return found

    def relay_copies(source, piece, kind, target):
        start, size = pieces[piece]
        part = pl.ds(start, size)
        found = [remote(kv.at[source, part], kv.at[source, part], send.at[source, piece, kind], recv.at[source, piece], target)]
        if piece == 1:
            found.append(remote(posb.at[source], posb.at[source], psend.at[source, kind], precv.at[source], target))
        return found

    def start_all(copies):
        for one in copies:
            one.start()

    def end_sends(copies):
        for one in copies:
            one.wait_send()

    def arrived(source, piece):
        for one in relay_copies(source, piece, 0, partner):
            one.wait_recv()

    def own_routes(act):
        for piece in (1, 2, 0):
            act(own_copies(piece, 2, across))
            pl.when(has_ahead)(lambda: act(own_copies(piece, 0, ahead)))
            pl.when(has_behind)(lambda: act(own_copies(piece, 1, behind)))
            act(own_copies(piece, 3, partner))

    directions = ((1, has_ahead, ahead), (-1, has_behind, behind))

    def at_distance(step, run):
        for way, onward, target in directions:
            far = z - way * step
            pl.when((far >= 0) & (far < line))(functools.partial(run, far, onward, target))

    def along(step, act, wait):
        def run(far, onward, target):
            source = index(far, lane, core)
            for piece in (1, 2):
                if wait:
                    arrived(source, piece)
                pl.when(onward)(lambda: act(relay_copies(source, piece, 0, target)))
                act(relay_copies(source, piece, 1, across))
                act(relay_copies(source, piece, 2, partner))
        at_distance(step, run)

    def along_short(step, act, wait):
        def run(far, onward, target):
            for yy in (lane, 1 - lane):
                source = index(far, yy, core)
                if wait:
                    arrived(source, 0)
                pl.when(onward)(lambda: act(relay_copies(source, 0, 0, target)))
                act(relay_copies(source, 0, 2, partner))
        at_distance(step, run)

    def crossed(source, act, wait):
        for piece in (1, 2):
            if wait:
                arrived(source, piece)
            act(relay_copies(source, piece, 2, partner))

    def crossed_here(act, wait):
        if wait:
            arrived(across, 0)
        pl.when(has_ahead)(lambda: act(relay_copies(across, 0, 0, ahead)))
        pl.when(has_behind)(lambda: act(relay_copies(across, 0, 1, behind)))
        act(relay_copies(across, 0, 2, partner))
        crossed(across, act, wait)

    def crossed_far(step, act, wait):
        at_distance(step, lambda far, onward, target: crossed(index(far, 1 - lane, core), act, wait))

    def attend(keys_of, values_of, key_pos):
        low = low_ref[...]
        high = high_ref[...]
        bias = []
        for g in range(2):
            here = key_pos(g)
            bias.append(jnp.where((here >= low) & (here <= high), 0.0, -1e30))
        bias = jnp.concatenate(bias, axis=1)
        for h in range(heads):
            column = pl.ds(h * HEAD_DIM, HEAD_DIM)
            scores = lax.dot_general(
                q_ref[:, column], keys_of(h), (((1,), (1,)), ((), ())), preferred_element_type=jnp.float32
            ) + bias
            before = top[h]
            now = jnp.maximum(before, jnp.max(scores, axis=1, keepdims=True))
            weights = jnp.exp2((scores - jnp.concatenate([now] * (rows // HEAD_DIM), axis=1)) * factor)
            fade = jnp.exp2((before - now) * factor)
            top[h] = now
            total[h] = total[h] * fade + jnp.sum(weights, axis=1, keepdims=True)
            acc[:, column] = acc[:, column] * fade + jnp.dot(
                weights.astype(jnp.bfloat16), values_of(h), preferred_element_type=jnp.float32
            )

    def attend_stored(source):
        attend(
            lambda h: kv[source, :, pl.ds(h * HEAD_DIM, HEAD_DIM)],
            lambda h: kv[source, :, pl.ds(cols + h * HEAD_DIM, HEAD_DIM)],
            lambda g: posb[source, pl.ds(g, 1), :],
        )

    def attend_second(source):
        for piece in range(3):
            arrived(source, piece)
        attend_stored(source)

    def attend_far(step):
        def run(far, onward, target):
            def one(j, carry):
                yy = lax.rem(lane + j, 2)
                attend_stored(index(far, yy, core))
                attend_second(index(far, yy, 1 - core))
                return carry
            lax.fori_loop(0, 2, one, 0)
        at_distance(step, run)

    own_routes(start_all)
    top[...] = jnp.full_like(top, -1e30)
    total[...] = jnp.zeros_like(total)
    acc[...] = jnp.zeros_like(acc)
    attend(
        lambda h: k_ref[:, pl.ds(h * HEAD_DIM, HEAD_DIM)],
        lambda h: v_ref[:, pl.ds(h * HEAD_DIM, HEAD_DIM)],
        lambda g: pos_ref[pl.ds(g, 1), :],
    )
    attend_second(partner)

    along(1, start_all, True)
    crossed_here(start_all, True)
    along_short(1, start_all, True)
    attend_stored(across)
    attend_second(index(z, 1 - lane, 1 - core))

    def loop(step, carry):
        along(step, start_all, True)
        along_short(step, start_all, True)
        crossed_far(step - 1, start_all, True)
        attend_far(step - 1)
        return carry

    lax.fori_loop(2, line + 1, loop, 0)

    for h in range(heads):
        column = pl.ds(h * HEAD_DIM, HEAD_DIM)
        out_ref[:, column] = (acc[:, column] / total[h]).astype(out_ref.dtype)

    own_routes(end_sends)
    crossed_here(end_sends, False)

    def drain(step, carry):
        along(step, end_sends, False)
        along_short(step, end_sends, False)
        crossed_far(step, end_sends, False)
        return carry

    lax.fori_loop(1, line, drain, 0)


def solution(mesh):
    members = mesh.shape["blk"]
    line = members // (CORES * LANES)

    def shards(queries, keys, values, group_table, doc_ids):
        rows, cols = queries.shape
        group = rows // 2
        heads = cols // HEAD_DIM
        within = jnp.arange(group, dtype=jnp.int32)
        groups = group_table.reshape(-1)
        positions = groups[:, None] * group + within[None, :]
        query_pos = positions.reshape(-1)
        query_doc = doc_ids.reshape(-1, group)[groups].reshape(-1)
        first = jnp.sum((doc_ids[None, :] < query_doc[:, None]).astype(jnp.int32), axis=1)
        low = jnp.broadcast_to(first[:, None], (rows, 128))
        high = jnp.broadcast_to(query_pos[:, None], (rows, 128))
        tile = jnp.concatenate([positions] * 4, axis=0)
        vmem = pl.BlockSpec(memory_space=pltpu.VMEM)
        return pl.pallas_call(
            functools.partial(attend_kernel, line),
            out_shape=jax.ShapeDtypeStruct((rows, cols), jnp.bfloat16),
            in_specs=[vmem] * 6,
            out_specs=vmem,
            scratch_shapes=[
                pltpu.VMEM((members, rows, 2 * cols), jnp.bfloat16),
                pltpu.VMEM((members, 8, 128), jnp.int32),
                pltpu.VMEM((heads, rows, HEAD_DIM), jnp.float32),
                pltpu.VMEM((heads, rows, HEAD_DIM), jnp.float32),
                pltpu.VMEM((rows, cols), jnp.float32),
                pltpu.SemaphoreType.DMA((members, 3)),
                pltpu.SemaphoreType.DMA((members,)),
                pltpu.SemaphoreType.DMA((3, 2, 4)),
                pltpu.SemaphoreType.DMA((4,)),
                pltpu.SemaphoreType.DMA((members, 3, 3)),
                pltpu.SemaphoreType.DMA((members, 3)),
            ],
            compiler_params=pltpu.CompilerParams(
                collective_id=0, has_side_effects=True, vmem_limit_bytes=60 * 1024 * 1024
            ),
        )(queries, keys, values, tile, low, high)

    in_specs = (P("blk", "head"), P("blk", "head"), P("blk", "head"), P("blk", None), P())
    return jax.shard_map(shards, mesh=mesh, in_specs=in_specs, out_specs=P("blk", "head"), check_vma=False)
```

```python
import functools
import math

import jax
import jax.numpy as jnp
from jax import lax
from jax.experimental import pallas as pl
from jax.experimental.pallas import tpu as pltpu
from jax.sharding import PartitionSpec as P

HEAD_DIM = 128
CORES = 2
LANES = 2


def attend_kernel(
    line, table_ref, q_hbm, k_hbm, v_hbm, table_hbm, doc_ref, out_ref,
    kv, posb, q_ref, low_ref, high_ref, top, total, acc, recv, precv, send, psend, load,
):
    rows, cols = k_hbm.shape
    heads = cols // HEAD_DIM
    group = rows // 2
    factor = math.log2(math.e) / math.sqrt(HEAD_DIM)
    me = lax.axis_index("blk")
    core = lax.rem(me, CORES)
    lane = lax.rem(me // CORES, LANES)
    z = me // (CORES * LANES)

    def index(zz, yy, cc):
        return (zz * LANES + yy) * CORES + cc

    across = index(z, 1 - lane, core)
    partner = index(z, lane, 1 - core)
    ahead = index(z + 1, lane, core)
    behind = index(z - 1, lane, core)
    has_ahead = z + 1 < line
    has_behind = z >= 1

    short = rows // 8
    half = (rows - short) // 2
    pieces = ((0, short), (short, half), (short + half, half))

    loads = (
        pltpu.make_async_copy(k_hbm, kv.at[me, :, pl.ds(0, cols)], load.at[0]),
        pltpu.make_async_copy(v_hbm, kv.at[me, :, pl.ds(cols, cols)], load.at[1]),
        pltpu.make_async_copy(table_hbm, posb.at[me], load.at[2]),
        pltpu.make_async_copy(q_hbm, q_ref, load.at[3]),
    )
    for one in loads:
        one.start()

    barrier = pltpu.get_barrier_semaphore()

    def greet(target):
        pl.semaphore_signal(barrier, inc=1, device_id={"blk": target})

    greet(across)
    greet(partner)
    pl.when(has_ahead)(lambda: greet(ahead))
    pl.when(has_behind)(lambda: greet(behind))
    pl.semaphore_wait(barrier, 2 + has_ahead.astype(jnp.int32) + has_behind.astype(jnp.int32))

    def remote(src, dst, ssem, rsem, target):
        return pltpu.make_async_remote_copy(
            src_ref=src, dst_ref=dst, send_sem=ssem, recv_sem=rsem, device_id={"blk": target}
        )

    def relay_copies(source, piece, kind, target):
        start, size = pieces[piece]
        part = pl.ds(start, size)
        found = [remote(kv.at[source, part], kv.at[source, part], send.at[source, piece, kind], recv.at[source, piece], target)]
        if piece == 1:
            found.append(remote(posb.at[source], posb.at[source], psend.at[source, kind], precv.at[source], target))
        return found

    def start_all(copies):
        for one in copies:
            one.start()

    def end_sends(copies):
        for one in copies:
            one.wait_send()

    def arrived(source, piece):
        for one in relay_copies(source, piece, 0, partner):
            one.wait_recv()

    def own_routes(act):
        for piece in (1, 2, 0):
            act(relay_copies(me, piece, 2, across))
            pl.when(has_ahead)(lambda: act(relay_copies(me, piece, 0, ahead)))
            pl.when(has_behind)(lambda: act(relay_copies(me, piece, 1, behind)))
            act(relay_copies(me, piece, 3, partner))

    directions = ((1, has_ahead, ahead), (-1, has_behind, behind))

    def at_distance(step, run):
        for way, onward, target in directions:
            far = z - way * step
            pl.when((far >= 0) & (far < line))(functools.partial(run, far, onward, target))

    def along(step, act, wait):
        def run(far, onward, target):
            source = index(far, lane, core)
            for piece in (1, 2):
                if wait:
                    arrived(source, piece)
                pl.when(onward)(lambda: act(relay_copies(source, piece, 0, target)))
                act(relay_copies(source, piece, 1, across))
                act(relay_copies(source, piece, 2, partner))
        at_distance(step, run)

    def along_short(step, act, wait):
        def run(far, onward, target):
            for yy in (lane, 1 - lane):
                source = index(far, yy, core)
                if wait:
                    arrived(source, 0)
                pl.when(onward)(lambda: act(relay_copies(source, 0, 0, target)))
                act(relay_copies(source, 0, 2, partner))
        at_distance(step, run)

    def crossed(source, act, wait):
        for piece in (1, 2):
            if wait:
                arrived(source, piece)
            act(relay_copies(source, piece, 2, partner))

    def crossed_here(act, wait):
        if wait:
            arrived(across, 0)
        pl.when(has_ahead)(lambda: act(relay_copies(across, 0, 0, ahead)))
        pl.when(has_behind)(lambda: act(relay_copies(across, 0, 1, behind)))
        act(relay_copies(across, 0, 2, partner))
        crossed(across, act, wait)

    def crossed_far(step, act, wait):
        at_distance(step, lambda far, onward, target: crossed(index(far, 1 - lane, core), act, wait))

    def attend(keys_of, values_of, key_pos):
        low = low_ref[...]
        high = high_ref[...]
        within = lax.broadcasted_iota(jnp.int32, (1, group), 1)
        bias = []
        for g in range(2):
            here = key_pos(g) * group + within
            bias.append(jnp.where((here >= low) & (here <= high), 0.0, -1e30))
        bias = jnp.concatenate(bias, axis=1)
        for h in range(heads):
            column = pl.ds(h * HEAD_DIM, HEAD_DIM)
            scores = lax.dot_general(
                q_ref[:, column], keys_of(h), (((1,), (1,)), ((), ())), preferred_element_type=jnp.float32
            ) + bias
            before = top[h]
            now = jnp.maximum(before, jnp.max(scores, axis=1, keepdims=True))
            weights = jnp.exp2((scores - jnp.concatenate([now] * (rows // HEAD_DIM), axis=1)) * factor)
            fade = jnp.exp2((before - now) * factor)
            top[h] = now
            total[h] = total[h] * fade + jnp.sum(weights, axis=1, keepdims=True)
            acc[:, column] = acc[:, column] * fade + jnp.dot(
                weights.astype(jnp.bfloat16), values_of(h), preferred_element_type=jnp.float32
            )

    def attend_stored(source):
        attend(
            lambda h: kv[source, :, pl.ds(h * HEAD_DIM, HEAD_DIM)],
            lambda h: kv[source, :, pl.ds(cols + h * HEAD_DIM, HEAD_DIM)],
            lambda g: posb[source][:, g:g + 1],
        )

    def attend_second(source):
        for piece in range(3):
            arrived(source, piece)
        attend_stored(source)

    def attend_far(step):
        def run(far, onward, target):
            def one(j, carry):
                yy = lax.rem(lane + j, 2)
                attend_stored(index(far, yy, core))
                attend_second(index(far, yy, 1 - core))
                return carry
            lax.fori_loop(0, 2, one, 0)
        at_distance(step, run)

    for one in loads:
        one.wait()
    own_routes(start_all)
    top[...] = jnp.full_like(top, -1e30)
    total[...] = jnp.zeros_like(total)
    acc[...] = jnp.zeros_like(acc)
    down = lax.broadcasted_iota(jnp.int32, (group, group), 0)
    right = lax.broadcasted_iota(jnp.int32, (group, group), 1)
    for g in range(2):
        own_group = table_ref[0, g]
        own_doc = jnp.broadcast_to(doc_ref[pl.ds(own_group, 1), :], (group, group))
        own_doc = jnp.sum(jnp.where(down == right, own_doc, 0), axis=1, keepdims=True)

        def count(i, found):
            return found + (doc_ref[pl.ds(i, 1), :] < own_doc).astype(jnp.int32)

        found = lax.fori_loop(0, doc_ref.shape[0], count, jnp.zeros((group, group), jnp.int32))
        part = pl.ds(g * group, group)
        low_ref[part, :] = jnp.broadcast_to(jnp.sum(found, axis=1, keepdims=True), (group, group))
        high_ref[part, :] = own_group * group + down
    attend_stored(me)
    attend_second(partner)

    along(1, start_all, True)
    crossed_here(start_all, True)
    along_short(1, start_all, True)
    attend_stored(across)
    attend_second(index(z, 1 - lane, 1 - core))

    def loop(step, carry):
        along(step, start_all, True)
        along_short(step, start_all, True)
        crossed_far(step - 1, start_all, True)
        attend_far(step - 1)
        return carry

    lax.fori_loop(2, line + 1, loop, 0)

    for h in range(heads):
        column = pl.ds(h * HEAD_DIM, HEAD_DIM)
        out_ref[:, column] = (acc[:, column] / total[h]).astype(out_ref.dtype)

    own_routes(end_sends)
    crossed_here(end_sends, False)

    def drain(step, carry):
        along(step, end_sends, False)
        along_short(step, end_sends, False)
        crossed_far(step, end_sends, False)
        return carry

    lax.fori_loop(1, line, drain, 0)


def solution(mesh):
    members = mesh.shape["blk"]
    line = members // (CORES * LANES)

    def shards(queries, keys, values, group_table, doc_ids):
        rows, cols = queries.shape
        group = rows // 2
        heads = cols // HEAD_DIM
        doc_rows = doc_ids.reshape(-1, group)
        vmem = pl.BlockSpec(memory_space=pltpu.VMEM)
        return pl.pallas_call(
            functools.partial(attend_kernel, line),
            out_shape=jax.ShapeDtypeStruct((rows, cols), jnp.bfloat16),
            in_specs=[pl.BlockSpec(memory_space=pltpu.SMEM)] + [pl.BlockSpec(memory_space=pl.ANY)] * 4 + [vmem],
            out_specs=vmem,
            scratch_shapes=[
                pltpu.VMEM((members, rows, 2 * cols), jnp.bfloat16),
                pltpu.VMEM((members, 1, 2), jnp.int32),
                pltpu.VMEM((rows, cols), jnp.bfloat16),
                pltpu.VMEM((rows, group), jnp.int32),
                pltpu.VMEM((rows, group), jnp.int32),
                pltpu.VMEM((heads, rows, HEAD_DIM), jnp.float32),
                pltpu.VMEM((heads, rows, HEAD_DIM), jnp.float32),
                pltpu.VMEM((rows, cols), jnp.float32),
                pltpu.SemaphoreType.DMA((members, 3)),
                pltpu.SemaphoreType.DMA((members,)),
                pltpu.SemaphoreType.DMA((members, 3, 4)),
                pltpu.SemaphoreType.DMA((members, 4)),
                pltpu.SemaphoreType.DMA((4,)),
            ],
            compiler_params=pltpu.CompilerParams(
                collective_id=0, has_side_effects=True, vmem_limit_bytes=60 * 1024 * 1024
            ),
        )(group_table, queries, keys, values, group_table, doc_rows)

    in_specs = (P("blk", "head"), P("blk", "head"), P("blk", "head"), P("blk", None), P())
    return jax.shard_map(shards, mesh=mesh, in_specs=in_specs, out_specs=P("blk", "head"), check_vma=False)
```

```python
import functools
import math

import jax
import jax.numpy as jnp
from jax import lax
from jax.experimental import pallas as pl
from jax.experimental.pallas import tpu as pltpu
from jax.sharding import PartitionSpec as P

HEAD_DIM = 128
CORES = 2
LANES = 2


def attend_kernel(
    line, table_ref, q_hbm, k_hbm, v_hbm, table_hbm, doc_ref, out_ref,
    kv, posb, q_ref, low_ref, high_ref, top, total, acc, recv, precv, send, psend, load,
):
    rows, cols = k_hbm.shape
    heads = cols // HEAD_DIM
    group = rows // 2
    factor = math.log2(math.e) / math.sqrt(HEAD_DIM)
    me = lax.axis_index("blk")
    core = lax.rem(me, CORES)
    lane = lax.rem(me // CORES, LANES)
    z = me // (CORES * LANES)

    def index(zz, yy, cc):
        return (zz * LANES + yy) * CORES + cc

    across = index(z, 1 - lane, core)
    partner = index(z, lane, 1 - core)
    ahead = index(z + 1, lane, core)
    behind = index(z - 1, lane, core)
    has_ahead = z + 1 < line
    has_behind = z >= 1

    short = rows // 8
    half = (rows - short) // 2
    pieces = ((0, short), (short, half), (short + half, half))

    loads = (
        pltpu.make_async_copy(k_hbm, kv.at[me, :, pl.ds(0, cols)], load.at[0]),
        pltpu.make_async_copy(v_hbm, kv.at[me, :, pl.ds(cols, cols)], load.at[1]),
        pltpu.make_async_copy(table_hbm, posb.at[me], load.at[2]),
        pltpu.make_async_copy(q_hbm, q_ref, load.at[3]),
    )
    for one in loads:
        one.start()

    barrier = pltpu.get_barrier_semaphore()

    def greet(target):
        pl.semaphore_signal(barrier, inc=1, device_id={"blk": target})

    greet(across)
    greet(partner)
    pl.when(has_ahead)(lambda: greet(ahead))
    pl.when(has_behind)(lambda: greet(behind))
    pl.semaphore_wait(barrier, 2 + has_ahead.astype(jnp.int32) + has_behind.astype(jnp.int32))

    def remote(src, dst, ssem, rsem, target):
        return pltpu.make_async_remote_copy(
            src_ref=src, dst_ref=dst, send_sem=ssem, recv_sem=rsem, device_id={"blk": target}
        )

    def relay_copies(source, piece, kind, target):
        start, size = pieces[piece]
        part = pl.ds(start, size)
        found = [remote(kv.at[source, part], kv.at[source, part], send.at[source, piece, kind], recv.at[source, piece], target)]
        if piece == 1:
            found.append(remote(posb.at[source], posb.at[source], psend.at[source, kind], precv.at[source], target))
        return found

    def start_all(copies):
        for one in copies:
            one.start()

    def end_sends(copies):
        for one in copies:
            one.wait_send()

    def arrived(source, piece):
        for one in relay_copies(source, piece, 0, partner):
            one.wait_recv()

    def own_routes(act):
        for piece in (0, 1, 2):
            act(relay_copies(me, piece, 2, across))
            pl.when(has_ahead)(lambda: act(relay_copies(me, piece, 0, ahead)))
            pl.when(has_behind)(lambda: act(relay_copies(me, piece, 1, behind)))
            act(relay_copies(me, piece, 3, partner))

    directions = ((1, has_ahead, ahead), (-1, has_behind, behind))

    def at_distance(step, run):
        for way, onward, target in directions:
            far = z - way * step
            pl.when((far >= 0) & (far < line))(functools.partial(run, far, onward, target))

    def along(step, act, wait):
        def run(far, onward, target):
            source = index(far, lane, core)
            for piece in (1, 2):
                if wait:
                    arrived(source, piece)
                pl.when(onward)(lambda: act(relay_copies(source, piece, 0, target)))
                act(relay_copies(source, piece, 1, across))
                act(relay_copies(source, piece, 2, partner))
        at_distance(step, run)

    def along_short(step, act, wait):
        def run(far, onward, target):
            for yy in (lane, 1 - lane):
                source = index(far, yy, core)
                if wait:
                    arrived(source, 0)
                pl.when(onward)(lambda: act(relay_copies(source, 0, 0, target)))
                act(relay_copies(source, 0, 2, partner))
        at_distance(step, run)

    def crossed(source, act, wait):
        for piece in (1, 2):
            if wait:
                arrived(source, piece)
            act(relay_copies(source, piece, 2, partner))

    def crossed_short(act, wait):
        if wait:
            arrived(across, 0)
        pl.when(has_ahead)(lambda: act(relay_copies(across, 0, 0, ahead)))
        pl.when(has_behind)(lambda: act(relay_copies(across, 0, 1, behind)))
        act(relay_copies(across, 0, 2, partner))

    def crossed_far(step, act, wait):
        at_distance(step, lambda far, onward, target: crossed(index(far, 1 - lane, core), act, wait))

    def attend(keys_of, values_of, key_pos):
        low = low_ref[...]
        high = high_ref[...]
        within = lax.broadcasted_iota(jnp.int32, (1, group), 1)
        bias = []
        for g in range(2):
            here = key_pos(g) * group + within
            bias.append(jnp.where((here >= low) & (here <= high), 0.0, -1e30))
        bias = jnp.concatenate(bias, axis=1)
        for h in range(heads):
            column = pl.ds(h * HEAD_DIM, HEAD_DIM)
            scores = lax.dot_general(
                q_ref[:, column], keys_of(h), (((1,), (1,)), ((), ())), preferred_element_type=jnp.float32
            ) + bias
            before = top[h]
            now = jnp.maximum(before, jnp.max(scores, axis=1, keepdims=True))
            weights = jnp.exp2((scores - jnp.concatenate([now] * (rows // HEAD_DIM), axis=1)) * factor)
            fade = jnp.exp2((before - now) * factor)
            top[h] = now
            total[h] = total[h] * fade + jnp.sum(weights, axis=1, keepdims=True)
            acc[:, column] = acc[:, column] * fade + jnp.dot(
                weights.astype(jnp.bfloat16), values_of(h), preferred_element_type=jnp.float32
            )

    def attend_stored(source):
        attend(
            lambda h: kv[source, :, pl.ds(h * HEAD_DIM, HEAD_DIM)],
            lambda h: kv[source, :, pl.ds(cols + h * HEAD_DIM, HEAD_DIM)],
            lambda g: posb[source][:, g:g + 1],
        )

    def attend_second(source):
        for piece in range(3):
            arrived(source, piece)
        attend_stored(source)

    def attend_far(step):
        def run(far, onward, target):
            def one(j, carry):
                yy = lax.rem(lane + j, 2)
                attend_stored(index(far, yy, core))
                attend_second(index(far, yy, 1 - core))
                return carry
            lax.fori_loop(0, 2, one, 0)
        at_distance(step, run)

    for one in loads:
        one.wait()
    own_routes(start_all)
    top[...] = jnp.full_like(top, -1e30)
    total[...] = jnp.zeros_like(total)
    acc[...] = jnp.zeros_like(acc)
    down = lax.broadcasted_iota(jnp.int32, (group, group), 0)
    right = lax.broadcasted_iota(jnp.int32, (group, group), 1)
    for g in range(2):
        own_group = table_ref[0, g]
        own_doc = jnp.broadcast_to(doc_ref[pl.ds(own_group, 1), :], (group, group))
        own_doc = jnp.sum(jnp.where(down == right, own_doc, 0), axis=1, keepdims=True)

        def count(i, found):
            return found + (doc_ref[pl.ds(i, 1), :] < own_doc).astype(jnp.int32)

        found = lax.fori_loop(0, doc_ref.shape[0], count, jnp.zeros((group, group), jnp.int32))
        part = pl.ds(g * group, group)
        low_ref[part, :] = jnp.broadcast_to(jnp.sum(found, axis=1, keepdims=True), (group, group))
        high_ref[part, :] = own_group * group + down
    attend_stored(me)
    crossed_short(start_all, True)
    attend_second(partner)

    along(1, start_all, True)
    crossed(across, start_all, True)
    along_short(1, start_all, True)
    attend_stored(across)
    attend_second(index(z, 1 - lane, 1 - core))

    def loop(step, carry):
        along(step, start_all, True)
        along_short(step, start_all, True)
        crossed_far(step - 1, start_all, True)
        attend_far(step - 1)
        return carry

    lax.fori_loop(2, line + 1, loop, 0)

    for h in range(heads):
        column = pl.ds(h * HEAD_DIM, HEAD_DIM)
        out_ref[:, column] = (acc[:, column] / total[h]).astype(out_ref.dtype)

    own_routes(end_sends)
    crossed_short(end_sends, False)
    crossed(across, end_sends, False)

    def drain(step, carry):
        along(step, end_sends, False)
        along_short(step, end_sends, False)
        crossed_far(step, end_sends, False)
        return carry

    lax.fori_loop(1, line, drain, 0)


def solution(mesh):
    members = mesh.shape["blk"]
    line = members // (CORES * LANES)

    def shards(queries, keys, values, group_table, doc_ids):
        rows, cols = queries.shape
        group = rows // 2
        heads = cols // HEAD_DIM
        doc_rows = doc_ids.reshape(-1, group)
        vmem = pl.BlockSpec(memory_space=pltpu.VMEM)
        return pl.pallas_call(
            functools.partial(attend_kernel, line),
            out_shape=jax.ShapeDtypeStruct((rows, cols), jnp.bfloat16),
            in_specs=[pl.BlockSpec(memory_space=pltpu.SMEM)] + [pl.BlockSpec(memory_space=pl.ANY)] * 4 + [vmem],
            out_specs=vmem,
            scratch_shapes=[
                pltpu.VMEM((members, rows, 2 * cols), jnp.bfloat16),
                pltpu.VMEM((members, 1, 2), jnp.int32),
                pltpu.VMEM((rows, cols), jnp.bfloat16),
                pltpu.VMEM((rows, group), jnp.int32),
                pltpu.VMEM((rows, group), jnp.int32),
                pltpu.VMEM((heads, rows, HEAD_DIM), jnp.float32),
                pltpu.VMEM((heads, rows, HEAD_DIM), jnp.float32),
                pltpu.VMEM((rows, cols), jnp.float32),
                pltpu.SemaphoreType.DMA((members, 3)),
                pltpu.SemaphoreType.DMA((members,)),
                pltpu.SemaphoreType.DMA((members, 3, 4)),
                pltpu.SemaphoreType.DMA((members, 4)),
                pltpu.SemaphoreType.DMA((4,)),
            ],
            compiler_params=pltpu.CompilerParams(
                collective_id=0, has_side_effects=True, vmem_limit_bytes=60 * 1024 * 1024
            ),
        )(group_table, queries, keys, values, group_table, doc_rows)

    in_specs = (P("blk", "head"), P("blk", "head"), P("blk", "head"), P("blk", None), P())
    return jax.shard_map(shards, mesh=mesh, in_specs=in_specs, out_specs=P("blk", "head"), check_vma=False)
```
